16 devices in a mesh: dp: 2 (over y, z), wg: 8 (over x, core).
Axes of the slice: x: 4, y: 2, z: 1, core: 2. Of those that a mesh axis runs over, the one named last changes fastest.
The devices are a block of a 4x4x8 slice.
Arguments:
- hidden: bfloat16 [65536, 1024], P(('dp', 'wg')), parts along dimension 0
- choice: int32 [65536, 8], P(('dp', 'wg')), parts along dimension 0
- pre_scale: float32 [1024], replicated
- w_router: bfloat16 [1024, 32], replicated
- w_gelu: bfloat16 [32, 1024, 512], P(None, None, 'wg')
- w_linear: bfloat16 [32, 1024, 512], P(None, None, 'wg')
- w_down: bfloat16 [32, 512, 1024], P(None, 'wg')
- post_scale: float32 [1024], replicated
Outputs:
- output: bfloat16 [65536, 1024], P(('dp', 'wg')), parts along dimension 0
There are 2 independent parts. The reference program is written for one: setup_inputs(seed, part) draws one part's arguments, and reference() takes and returns one part's arrays. A program takes and returns all parts, laid end to end along the dimension named above; an argument that names none is the same for every part.
All inputs are finite; a program needn't handle non-finite values.
Results may differ from the reference program's by a relative error of at most 0.001.
Values are sent between devices in bfloat16 or wider.
A program may use at most 768 MiB of HBM per device.

```python
import jax
import jax.numpy as jnp
from jax import lax

D_MODEL = 1024
D_FF = 512
EXPERTS = 32
TOP_K = 8
TOKENS_DEV = 4096
GROUP_DEVS = 8
EPS = 1e-5


def block_choice(block_key):
    mean_load = TOKENS_DEV * TOP_K // EXPERTS
    key_perm, key_delta, key_rows = jax.random.split(block_key, 3)
    expert_perm = jax.random.permutation(key_perm, EXPERTS)
    pair_delta = jax.random.randint(key_delta, (EXPERTS,), 0, mean_load)
    position = jnp.arange(EXPERTS)
    pair_index = jnp.maximum((position - 3) // 2, 0)
    pair_sign = jnp.where((position - 3) % 2 == 0, 1, -1)
    paired = (position >= 3) & (4 + 2 * pair_index < EXPERTS)
    load_delta = jnp.where(paired, pair_sign * pair_delta[pair_index], 0)
    load_delta = load_delta + jnp.where(position == 0, mean_load, 0) - jnp.where((position == 1) | (position == 2), mean_load // 2, 0)
    expert_loads = mean_load + load_delta
    run_ends = jnp.cumsum(expert_loads)
    flat_pos = jnp.arange(TOKENS_DEV * TOP_K)
    run_index = jnp.sum((flat_pos[:, None] >= run_ends[None, :]).astype(jnp.int32), axis=1)
    choice_grid = expert_perm[run_index].reshape(TOP_K, TOKENS_DEV).T
    row_perm = jax.random.permutation(key_rows, TOKENS_DEV)
    return choice_grid[row_perm].astype(jnp.int32)


def setup_inputs(seed: int = 0, part: int = 0) -> dict:
    weight_keys = jax.random.split(jax.random.key(seed), 6)
    part_key = jax.random.fold_in(jax.random.key(seed + 1), part)
    key_hidden, key_choice = jax.random.split(part_key)
    row_count = GROUP_DEVS * TOKENS_DEV
    hidden = jax.random.normal(key_hidden, (row_count, D_MODEL), jnp.float32).astype(jnp.bfloat16)
    choice = jax.vmap(block_choice)(jax.random.split(key_choice, GROUP_DEVS)).reshape(row_count, TOP_K)
    pre_scale = 1.0 + 0.5 * jax.random.normal(weight_keys[0], (D_MODEL,), jnp.float32)
    w_router = (jax.random.normal(weight_keys[1], (D_MODEL, EXPERTS), jnp.float32) * D_MODEL ** -0.5).astype(jnp.bfloat16)
    w_gelu = (jax.random.normal(weight_keys[2], (EXPERTS, D_MODEL, D_FF), jnp.float32) * D_MODEL ** -0.5).astype(jnp.bfloat16)
    w_linear = (jax.random.normal(weight_keys[3], (EXPERTS, D_MODEL, D_FF), jnp.float32) * D_MODEL ** -0.5).astype(jnp.bfloat16)
    w_down = (jax.random.normal(weight_keys[4], (EXPERTS, D_FF, D_MODEL), jnp.float32) * D_FF ** -0.5).astype(jnp.bfloat16)
    post_scale = 1.0 + 0.5 * jax.random.normal(weight_keys[5], (D_MODEL,), jnp.float32)
    return dict(hidden=hidden, choice=choice, pre_scale=pre_scale, w_router=w_router, w_gelu=w_gelu, w_linear=w_linear, w_down=w_down, post_scale=post_scale)


def rms_norm(values, gain_vec):
    return values * lax.rsqrt(jnp.mean(values * values, axis=-1, keepdims=True) + EPS) * gain_vec


def route_slots(block_ids, capacity):
    tok_rows, top_k = block_ids.shape
    flat_ids = block_ids.reshape(-1)
    sort_order = jnp.argsort(flat_ids, stable=True)
    counts = jnp.sum((flat_ids[:, None] == jnp.arange(EXPERTS)[None, :]).astype(jnp.int32), axis=0)
    starts = jnp.cumsum(counts) - counts
    slot_rank = jnp.arange(capacity)
    source = jnp.minimum(starts[:, None] + slot_rank[None, :], tok_rows * top_k - 1)
    slot_token = sort_order[source].reshape(-1) // top_k
    sorted_pos = jnp.argsort(sort_order, stable=True)
    slot_of = flat_ids * capacity + sorted_pos - starts[flat_ids]
    return slot_token, slot_of


def reference(hidden, choice, pre_scale, w_router, w_gelu, w_linear, w_down, post_scale):
    capacity = 2 * TOKENS_DEV * TOP_K // EXPERTS
    hidden_f = hidden.astype(jnp.float32)
    normed = rms_norm(hidden_f, pre_scale).astype(jnp.bfloat16)
    router_probs = jax.nn.softmax(jnp.dot(normed, w_router, preferred_element_type=jnp.float32), axis=-1)
    gate_vals = jnp.take_along_axis(router_probs, choice, axis=1)

    def one_expert(expert_args):
        expert_rows, gelu_w, linear_w, down_w = expert_args
        gelu_in = jnp.dot(expert_rows, gelu_w, preferred_element_type=jnp.float32)
        linear_in = jnp.dot(expert_rows, linear_w, preferred_element_type=jnp.float32)
        hidden_act = (jax.nn.gelu(gelu_in, approximate=True) * linear_in).astype(jnp.bfloat16)
        return jnp.dot(hidden_act, down_w, preferred_element_type=jnp.float32)

    def one_block(block_args):
        block_rows, block_ids, block_gates = block_args
        slot_token, slot_of = route_slots(block_ids, capacity)
        dispatched = jnp.take(block_rows, slot_token, axis=0).reshape(EXPERTS, capacity, D_MODEL)
        expert_out = lax.map(one_expert, (dispatched, w_gelu, w_linear, w_down)).reshape(EXPERTS * capacity, D_MODEL)
        picked = jnp.take(expert_out, slot_of, axis=0).reshape(TOKENS_DEV, TOP_K, D_MODEL)
        return jnp.sum(picked * block_gates[:, :, None], axis=1)

    mixed_out = lax.map(one_block, (normed.reshape(GROUP_DEVS, TOKENS_DEV, D_MODEL), choice.reshape(GROUP_DEVS, TOKENS_DEV, TOP_K), gate_vals.reshape(GROUP_DEVS, TOKENS_DEV, TOP_K))).reshape(GROUP_DEVS * TOKENS_DEV, D_MODEL)
    return (hidden_f + rms_norm(mixed_out, post_scale)).astype(jnp.bfloat16)
```

```python
import functools

import jax
import jax.numpy as jnp
from jax import lax
from jax.experimental import pallas as pl
from jax.experimental.pallas import tpu as pltpu
from jax.sharding import PartitionSpec as P

EPS = 1e-5
LANES = 128
SUB = 8
TILE = 256
PRE_TILE = 1024
PRE_PART = 256
POST_TILE = 256
GROUP = 8
CHUNKS = (4, 6, 6, 6, 4, 3, 2, 1)
VMEM_LIMIT = 64 * 1024 * 1024 - 65536
NT = (((1,), (1,)), ((), ()))


def gate_pitch(t_rows):
    return t_rows + SUB * LANES


def pre_kernel(h_ref, gain_ref, wr_ref, x_ref, p_ref):
    rows, d_model = h_ref.shape
    for r0 in range(0, rows, PRE_PART):
        h = h_ref[r0:r0 + PRE_PART, :].astype(jnp.float32)
        scale = lax.rsqrt(jnp.mean(h * h, axis=-1, keepdims=True) + EPS)
        b = (h * scale * gain_ref[...]).astype(jnp.bfloat16)
        logits = lax.dot_general(wr_ref[...], b, NT, preferred_element_type=jnp.float32)
        peak = jnp.max(logits, axis=0, keepdims=True)
        e = jnp.exp(logits - peak)
        probs = e / jnp.sum(e, axis=0, keepdims=True)
        for j in range(PRE_PART // LANES):
            p_ref[:, r0 // LANES + j, :] = probs[:, j * LANES:(j + 1) * LANES]
        bf = b.astype(jnp.float32)
        for j in range(d_model // LANES):
            x_ref[pl.ds(r0 * SUB + j, PRE_PART, stride=SUB), :] = bf[:, j * LANES:(j + 1) * LANES]


def moe_kernel(first, last, e0, *refs):
    list_hbm, tstart_ref, gate_hbm, x_hbm, w_hbm = refs[:5]
    refs = refs[5:]
    if not first:
        y_in, refs = refs[0], refs[1:]
    if last:
        hid_hbm, post_ref, refs = refs[0], refs[1], refs[2:]
    y_out, refs = refs[0], refs[1:]
    list_ref, gate_ref, x_v, y_v, wg_v, wl_v, wd_v, xs, os_, xb, ab, wsem, xsem, ysem, lsem, gsem = refs[:16]
    if last:
        hbuf, obuf, hsem, osem = refs[16:]

    shards, _, e_c, f_dev, d_model = w_hbm.shape
    t_rows = x_hbm.shape[0] // SUB
    dff = shards * f_dev
    nj = d_model // LANES
    pitch = TILE + 1
    half = dff // 2

    def w_copies(e, slot):
        return [
            pltpu.make_async_copy(w_hbm.at[:, k, e], buf.at[slot], wsem.at[slot, k])
            for k, buf in enumerate((wg_v, wl_v, wd_v))
        ]

    t_begin = tstart_ref[e0]
    t_end = tstart_ref[e0 + e_c]
    span = list_ref.shape[0] // TILE
    tiles = list_hbm.shape[0] // TILE
    align = max(1, SUB * LANES // TILE)
    l_first = jnp.minimum(t_begin // align * align, tiles - span)
    l_copy = pltpu.make_async_copy(list_hbm.at[pl.ds(pl.multiple_of(l_first * TILE, align * TILE), span * TILE)], list_ref, lsem)
    g_copy = pltpu.make_async_copy(gate_hbm.at[pl.ds(e0 * gate_pitch(t_rows), e_c * gate_pitch(t_rows))], gate_ref, gsem)
    l_copy.start()
    g_copy.start()
    x_copy = pltpu.make_async_copy(x_hbm, x_v.at[pl.ds(0, t_rows * SUB)], xsem)
    x_copy.start()
    for c in w_copies(0, 0):
        c.start()
    if not first:
        y_copy = pltpu.make_async_copy(y_in, y_v, ysem)
        y_copy.start()
    else:
        def zero(i, _):
            y_v[pl.ds(pl.multiple_of(i * 64, 64), 64), :] = jnp.zeros((64, LANES), jnp.float32)
            return 0
        lax.fori_loop(0, y_v.shape[0] // 64, zero, 0)
    x_v[pl.ds(t_rows * SUB, SUB), :] = jnp.zeros((SUB, LANES), jnp.float32)
    l_copy.wait()
    g_copy.wait()
    x_copy.wait()

    def gather(tile):
        base = jnp.minimum(tile - l_first, span - 1) * TILE
        for m in range(TILE):
            t = list_ref[base + m]
            xs[pl.ds(m, SUB, stride=pitch), :] = x_v[pl.ds(pl.multiple_of(t * SUB, SUB), SUB), :]

    def combine(tile, e):
        base = (tile - l_first) * TILE
        gbase = e * gate_pitch(t_rows)
        for m0 in range(0, TILE, GROUP):
            toks, vals = [], []
            for m in range(m0, m0 + GROUP):
                t = list_ref[base + m]
                g = gate_ref[gbase + t]
                row = pl.ds(pl.multiple_of(t * SUB, SUB), SUB)
                toks.append(row)
                vals.append(y_v[row, :] + g * os_[pl.ds(m, SUB, stride=pitch), :])
            for row, val in zip(toks, vals):
                y_v[row, :] = val

    def matmuls(slot):
        for h in range(2):
            sh = shards // 2
            wg = wg_v[slot, h * sh:(h + 1) * sh].reshape(half, d_model)
            wl = wl_v[slot, h * sh:(h + 1) * sh].reshape(half, d_model)
            uv = lax.dot_general(xb[...], jnp.concatenate([wg, wl], axis=0), NT, preferred_element_type=jnp.float32)
            u, v = uv[:, :half], uv[:, half:]
            ab[:, h * half:(h + 1) * half] = (jax.nn.gelu(u, approximate=True) * v).astype(jnp.bfloat16)
        wd = wd_v[slot].reshape(dff, d_model)
        for n in range(2):
            width = d_model // 2
            o = jnp.dot(ab[...], wd[:, n * width:(n + 1) * width], preferred_element_type=jnp.float32)
            for j in range(width // LANES):
                os_[pl.ds((n * width // LANES + j) * pitch, TILE), :] = o[:, j * LANES:(j + 1) * LANES]

    def enter(e):
        slot = lax.rem(e, 2)
        for c in w_copies(e, slot):
            c.wait()

        @pl.when(e + 1 < e_c)
        def _():
            for c in w_copies(e + 1, 1 - slot):
                c.start()

    gather(t_begin)
    for j in range(nj):
        os_[pl.ds(j * pitch, TILE), :] = jnp.zeros((TILE, LANES), jnp.float32)
    enter(jnp.int32(0))
    if not first:
        y_copy.wait()

    def body(tile, e_prev):
        new = tile >= tstart_ref[e0 + e_prev + 1]
        e = e_prev + new.astype(jnp.int32)

        @pl.when(new)
        def _():
            enter(e)

        for j in range(nj):
            xb[:, j * LANES:(j + 1) * LANES] = xs[pl.ds(j * pitch, TILE), :].astype(jnp.bfloat16)
        gather(tile + 1)
        combine(jnp.maximum(tile - 1, t_begin), e_prev)
        matmuls(lax.rem(e, 2))
        return e

    e_last = lax.fori_loop(t_begin, t_end, body, jnp.int32(0))
    combine(t_end - 1, e_last)

    if not last:
        out = pltpu.make_async_copy(y_v, y_out, ysem)
        out.start()
        out.wait()
        return

    n_post = t_rows // POST_TILE

    def h_copy(i, slot):
        return pltpu.make_async_copy(hid_hbm.at[pl.ds(pl.multiple_of(i * POST_TILE, POST_TILE), POST_TILE)], hbuf.at[slot], hsem.at[slot])

    def o_copy(i, slot):
        return pltpu.make_async_copy(obuf.at[slot], y_out.at[pl.ds(pl.multiple_of(i * POST_TILE, POST_TILE), POST_TILE)], osem.at[slot])

    h_copy(0, 0).start()

    def post(i, _):
        slot = lax.rem(i, 2)

        @pl.when(i + 1 < n_post)
        def _():
            h_copy(i + 1, 1 - slot).start()

        @pl.when(i >= 2)
        def _():
            o_copy(i - 2, slot).wait()

        h_copy(i, slot).wait()
        parts = [y_v[pl.ds(i * POST_TILE * SUB + j, POST_TILE, stride=SUB), :] for j in range(nj)]
        square = parts[0] * parts[0]
        for part in parts[1:]:
            square = square + part * part
        scale = lax.rsqrt(jnp.sum(square, axis=-1, keepdims=True) / d_model + EPS)
        for j in range(nj):
            cols = slice(j * LANES, (j + 1) * LANES)
            val = hbuf[slot, :, cols].astype(jnp.float32) + parts[j] * scale * post_ref[:, cols]
            obuf[slot, :, cols] = val.astype(jnp.bfloat16)
        o_copy(i, slot).start()
        return 0

    lax.fori_loop(0, n_post, post, 0)
    for i in range(max(0, n_post - 2), n_post):
        o_copy(i, i % 2).wait()


def run_pre(hidden, pre_scale, w_router, interpret=False):
    t_rows, d_model = hidden.shape
    num_experts = w_router.shape[1]
    return pl.pallas_call(
        pre_kernel,
        grid=(t_rows // PRE_TILE,),
        in_specs=[
            pl.BlockSpec((PRE_TILE, d_model), lambda i: (i, 0)),
            pl.BlockSpec((1, d_model), lambda i: (0, 0)),
            pl.BlockSpec((num_experts, d_model), lambda i: (0, 0)),
        ],
        out_specs=[
            pl.BlockSpec((PRE_TILE * SUB, LANES), lambda i: (i, 0)),
            pl.BlockSpec((num_experts, PRE_TILE // LANES, LANES), lambda i: (0, i, 0)),
        ],
        out_shape=[
            jax.ShapeDtypeStruct((t_rows * SUB, LANES), jnp.float32),
            jax.ShapeDtypeStruct((num_experts, gate_pitch(t_rows) // LANES, LANES), jnp.float32),
        ],
        name='pre',
        interpret=interpret,
    )(hidden, pre_scale.reshape(1, d_model), w_router.T)


def run_moe(first, last, e0, lists, tstart, gates, x, w, y, hidden, post_scale, interpret=False):
    shards, _, e_c, f_dev, d_model = w.shape
    t_rows = x.shape[0] // SUB
    align = max(1, SUB * LANES // TILE)
    span = min(lists.shape[0] // TILE, e_c * (t_rows // 2 // TILE) + align)
    y_rows = (t_rows + SUB) * SUB
    dff = shards * f_dev
    smem = pl.BlockSpec(memory_space=pltpu.SMEM)
    hbm = pl.BlockSpec(memory_space=pl.ANY)
    args = [lists, tstart, gates, x, w]
    specs = [hbm, smem, hbm, hbm, hbm]
    aliases = {}
    if not first:
        if not last:
            aliases = {len(args): 0}
        args.append(y)
        specs.append(hbm)
    scratch = [
        pltpu.SMEM((span * TILE,), jnp.int32),
        pltpu.SMEM((e_c * gate_pitch(t_rows),), jnp.float32),
        pltpu.VMEM((y_rows, LANES), jnp.float32),
        pltpu.VMEM((y_rows, LANES), jnp.float32),
        pltpu.VMEM((2, shards, f_dev, d_model), jnp.bfloat16),
        pltpu.VMEM((2, shards, f_dev, d_model), jnp.bfloat16),
        pltpu.VMEM((2, shards, f_dev, d_model), jnp.bfloat16),
        pltpu.VMEM((SUB * (TILE + 1), LANES), jnp.float32),
        pltpu.VMEM((SUB * (TILE + 1), LANES), jnp.float32),
        pltpu.VMEM((TILE, d_model), jnp.bfloat16),
        pltpu.VMEM((TILE, dff), jnp.bfloat16),
        pltpu.SemaphoreType.DMA((2, 3)),
        pltpu.SemaphoreType.DMA,
        pltpu.SemaphoreType.DMA,
        pltpu.SemaphoreType.DMA,
        pltpu.SemaphoreType.DMA,
    ]
    if last:
        args += [hidden, post_scale.reshape(1, d_model)]
        specs += [hbm, pl.BlockSpec(memory_space=pltpu.VMEM)]
        out_shape = jax.ShapeDtypeStruct((t_rows, d_model), jnp.bfloat16)
        scratch += [
            pltpu.VMEM((2, POST_TILE, d_model), jnp.bfloat16),
            pltpu.VMEM((2, POST_TILE, d_model), jnp.bfloat16),
            pltpu.SemaphoreType.DMA((2,)),
            pltpu.SemaphoreType.DMA((2,)),
        ]
    else:
        out_shape = jax.ShapeDtypeStruct((y_rows, LANES), jnp.float32)
    rows = e_c * 1024
    return pl.pallas_call(
        functools.partial(moe_kernel, first, last, e0),
        in_specs=specs,
        out_specs=hbm,
        out_shape=out_shape,
        scratch_shapes=scratch,
        input_output_aliases=aliases,
        compiler_params=pltpu.CompilerParams(vmem_limit_bytes=VMEM_LIMIT),
        cost_estimate=pl.CostEstimate(flops=rows * 6 * d_model * dff, bytes_accessed=3 * y_rows * LANES * 4 + w.size * 2, transcendentals=0),
        name=f'moe_{e0}',
        interpret=interpret,
    )(*args)


def make_lists(choice_t, num_experts):
    top_k, t_rows = choice_t.shape
    big = 2 * t_rows
    keys = choice_t * big + lax.broadcasted_iota(jnp.int32, choice_t.shape, 1)
    experts = lax.broadcasted_iota(jnp.int32, (num_experts, 1, 1), 0)
    counts = jnp.sum((choice_t[None] == experts).astype(jnp.int32), axis=(1, 2))
    tiles = (counts + TILE - 1) // TILE
    pad = tiles * TILE - counts
    slot = lax.broadcasted_iota(jnp.int32, (num_experts, TILE), 1)
    owner = lax.broadcasted_iota(jnp.int32, (num_experts, TILE), 0)
    fill = jnp.where(slot < pad[:, None], owner, num_experts) * big + t_rows
    ordered = lax.sort(jnp.concatenate([keys.reshape(-1), fill.reshape(-1)]), is_stable=False)
    lists = ordered & (big - 1)
    tstart = jnp.concatenate([jnp.zeros((1,), jnp.int32), jnp.cumsum(tiles)])
    return lists, tstart


def solution(mesh):
    def local_block(hidden, choice, pre_scale, w_router, w_gelu, w_linear, w_down, post_scale):
        t_rows, d_model = hidden.shape
        num_experts = w_gelu.shape[0]
        gelu_t = jnp.swapaxes(w_gelu, 1, 2)
        linear_t = jnp.swapaxes(w_linear, 1, 2)
        weights = []
        e0 = 0
        for e_c in CHUNKS:
            part = jnp.stack([gelu_t[e0:e0 + e_c], linear_t[e0:e0 + e_c], w_down[e0:e0 + e_c]], axis=0)
            weights.append(lax.all_gather(part, 'wg', axis=0, tiled=False))
            e0 += e_c
        x, p = run_pre(hidden, pre_scale, w_router)
        gates = p.reshape(-1)
        lists, tstart = make_lists(choice.T, num_experts)
        y = None
        e0 = 0
        for c, e_c in enumerate(CHUNKS):
            y = run_moe(c == 0, c == len(CHUNKS) - 1, e0, lists, tstart, gates, x, weights[c], y, hidden, post_scale)
            e0 += e_c
        return y

    row_spec = P(('dp', 'wg'), None)
    weight_in = P(None, None, 'wg')
    return jax.shard_map(local_block, mesh=mesh, in_specs=(row_spec, row_spec, P(), P(), weight_in, weight_in, P(None, 'wg', None), P()), out_specs=row_spec, check_vma=False)
```
